32 devices in a mesh: seq: 8 (over z, core), tp: 2 (over y), dp: 2 (over x).
Axes of the slice: x: 2, y: 2, z: 4, core: 2. Of those that a mesh axis runs over, the one named last changes fastest.
Arguments:
- query_latent: bfloat16 [2, 2048, 1536], P('dp', 'seq', 'tp'), may hold values from -6 to 6
- key_latent: bfloat16 [2, 2048, 512], P('dp', 'seq', 'tp'), may hold values from -6 to 6
- rope_key: bfloat16 [2, 2048, 64], P('dp', 'seq'), may hold values from -6 to 6
- w_uq: bfloat16 [1536, 12288], P('seq', 'tp')
- w_uk: bfloat16 [512, 8192], P('seq', 'tp'), may hold values from -0.25 to 0.25
- w_uv: bfloat16 [512, 8192], P('seq', 'tp'), may hold values from -0.25 to 0.25
- block_order: int32 [2, 16], P('dp'), may hold values from 0 to 15, each once within a row
- segment_ids: int32 [2, 2048], P('dp'), may hold values from 0 to 3, never falling along the last dimension, each value on 1 to 1024 neighbouring positions
Outputs:
- context: bfloat16 [2, 2048, 8192], P('dp', 'seq', 'tp')
- clipped_uq: bfloat16 [1536, 12288], P('seq', 'tp')
- clipped_uk: bfloat16 [512, 8192], P('seq', 'tp')
The draws below stay inside these ranges and needn't reach their ends.
Inputs may be any that keep to these rules, and one draw needn't show every extreme that they name: `block_order`: each row is a permutation of the 16 position blocks. `segment_ids`: never falling along positions; each document has at most 1024 positions.
All inputs are finite; a program needn't handle non-finite values.
Results may differ from the reference program's by a relative error of at most 0.012.
The reference program's roundings to bfloat16 on the way (of `weights`) count: a program that leaves them out, or rounds other values in their place, can miss the bound.
Values may be sent and summed in bfloat16 or wider, within the bound.
A program may use at most 128 MiB of HBM per device.

```python
import math
import jax
import jax.numpy as jnp
import numpy as np
from jax import lax

HEADS = 64
NOPE = 128
ROPE = 64
VD = 128
QL = 1536
KL = 512
TOK_DEV = 256
CLIP = 8
L = 2048
BLOCKS = 16
SEQS = 2
N_DP = 2


def draw_w_uq(key, part):
    first, second = jax.random.split(jax.random.fold_in(key, 11))
    base = jax.random.normal(first, (QL, HEADS * (NOPE + ROPE)), jnp.float32) * QL ** (-0.5)
    lowest, highest = (math.log(0.5), math.log(3.0))
    exponent = jax.random.uniform(second, (HEADS,), jnp.float32, lowest, highest)
    factor = jnp.repeat(jnp.exp(exponent), NOPE + ROPE)
    return (base * factor[None, :]).astype(jnp.bfloat16)


def shard_levels(stream_key, shape, pieces, least, top_value):
    def one(axis_at, blocks):
        draws = jax.random.uniform(jax.random.fold_in(jax.random.fold_in(stream_key, 6), axis_at), (blocks,), jnp.float32, least / len(pieces), top_value / len(pieces))
        return jnp.repeat(jnp.exp(draws), shape[axis_at] // blocks).reshape((-1,) + (1,) * (len(shape) - axis_at - 1))

    level = one(*pieces[0])
    for cut in pieces[1:]:
        level = level * one(*cut)
    return level


def length_profile(amount, total, reach, slope):
    portions = [(1 << 20) // math.isqrt(rank ** slope) + 1 for rank in range(2, amount + 1)]
    rest, counts = total - reach - (amount - 1), [1] * (amount - 1)
    while rest > 0:
        free = [i for i in range(amount - 1) if counts[i] < reach]
        pool, remaining = sum([portions[i] for i in free]), rest
        for i in free:
            extra = min(reach - counts[i], max(1, remaining * portions[i] // pool), rest)
            counts[i] = counts[i] + extra
            rest = rest - extra
    return np.array([reach] + counts)


def ragged(own_key, number_of, total, limit, slope):
    if number_of == 2:
        one = jax.random.randint(own_key, (), max(1, total - limit), min(limit, total - 1) + 1)
        return jnp.stack([one, total - one])
    lengths = jnp.asarray(length_profile(number_of, total, limit, slope), jnp.int32)
    twos = (number_of - 1) // 2
    giver, taker = lengths[1:1 + 2 * twos:2], lengths[2:2 + 2 * twos:2]
    room = jnp.minimum(giver - 1, limit - taker)
    moved = jax.random.randint(jax.random.fold_in(own_key, 1), (twos,), 0, 1 << 20) % (room + 1)
    lengths = lengths.at[1:1 + 2 * twos:2].set(giver - moved).at[2:2 + 2 * twos:2].set(taker + moved)
    return lengths[jax.random.permutation(jax.random.fold_in(own_key, 2), number_of)]


def centred(rng, extent, deviation, bound, cuts=(), kind=jnp.bfloat16):
    level = shard_levels(rng, extent, cuts, -0.22, 0.18) if cuts else 1.0
    drawn = jax.random.normal(rng, extent, jnp.float32) * deviation * level
    return jnp.minimum(jnp.maximum(drawn, -bound), bound).astype(kind)


def setup_inputs(seed: int = 0) -> dict:
    splits = jax.random.split(jax.random.key(seed), 9)
    query_latent = centred(splits[0], (SEQS, L, QL), 1.0, 6.0, ((0, 2), (1, 8), (2, 2)))
    key_latent = centred(splits[1], (SEQS, L, KL), 1.0, 6.0, ((0, 2), (1, 8), (2, 2)))
    rope_key = centred(splits[2], (SEQS, L, ROPE), 1.0, 6.0, ((0, 2), (1, 8)))
    w_uq = draw_w_uq(jax.random.fold_in(splits[8], 71), 0)
    w_uk = centred(splits[4], (KL, HEADS * NOPE), KL ** -0.5, 0.25, ((0, 8), (1, 2)))
    w_uv = centred(splits[5], (KL, HEADS * VD), KL ** -0.5, 0.25, ((0, 8), (1, 2)))
    block_order = jax.vmap(lambda own: jax.random.permutation(own, BLOCKS))(jax.random.split(splits[6], SEQS)).reshape((SEQS, BLOCKS)).astype(jnp.int32)
    segment_ids = jax.vmap(lambda own: jnp.searchsorted(jnp.cumsum(ragged(own, 4, L, L // 2, 1)), jnp.arange(L), side="right"))(jax.random.split(splits[7], SEQS)).reshape((SEQS, L)).astype(jnp.int32)
    return {"query_latent": query_latent, "key_latent": key_latent, "rope_key": rope_key, "w_uq": w_uq, "w_uk": w_uk, "w_uv": w_uv, "block_order": block_order, "segment_ids": segment_ids}


rope_base = 50000.0
masked_value = -1e+30

def turning(positions, width):
    steps = jnp.arange(width // 2, dtype=jnp.float32) * (2.0 / width)
    freqs = jnp.exp(-math.log(rope_base) * steps)
    angle = positions.astype(jnp.float32)[:, None] * freqs[None, :]
    return (jnp.cos(angle), jnp.sin(angle))

def rotate(values, cosine, sine):
    half = values.shape[-1] // 2
    first = values[..., :half]
    second = values[..., half:]
    return jnp.concatenate([first * cosine - second * sine, second * cosine + first * sine], axis=-1)

def stored_positions(order, half_block):
    count = order.shape[0] * half_block
    index = jnp.arange(count, dtype=jnp.int32)
    return (jnp.take(order, index // half_block) * half_block + index % half_block).astype(jnp.int32)

def reference(query_latent, key_latent, rope_key, w_uq, w_uk, w_uv, block_order, segment_ids):
    half_block = TOK_DEV // 2
    scale = 1.0 / math.sqrt(NOPE + ROPE)
    contexts = []
    largest = jnp.full((HEADS,), masked_value, jnp.float32)
    for member in range(N_DP):
        positions = stored_positions(block_order[member], half_block)
        labels = jnp.take(segment_ids[member], positions)
        cosine, sine = turning(positions, ROPE)
        query_full = jnp.dot(query_latent[member], w_uq, preferred_element_type=jnp.float32).reshape(L, HEADS, NOPE + ROPE)
        query_nope = query_full[:, :, :NOPE].astype(jnp.bfloat16)
        query_rope = rotate(query_full[:, :, NOPE:], cosine[:, None, :], sine[:, None, :]).astype(jnp.bfloat16)
        key_nope = jnp.dot(key_latent[member], w_uk, preferred_element_type=jnp.float32).astype(jnp.bfloat16).reshape(L, HEADS, NOPE)
        values = jnp.dot(key_latent[member], w_uv, preferred_element_type=jnp.float32).astype(jnp.bfloat16).reshape(L, HEADS, VD)
        key_rope = rotate(rope_key[member].astype(jnp.float32), cosine, sine).astype(jnp.bfloat16)
        allowed = (positions[None, :] <= positions[:, None]) & (labels[None, :] == labels[:, None])

        def one_head(inputs):
            head_qn, head_qr, head_kn, head_values = inputs
            scores = jnp.dot(head_qn, head_kn.T, preferred_element_type=jnp.float32)
            scores = (scores + jnp.dot(head_qr, key_rope.T, preferred_element_type=jnp.float32)) * scale
            masked = jnp.where(allowed, scores, masked_value)
            row_max = lax.optimization_barrier(jnp.max(masked, axis=1))
            weights = jnp.where(allowed, jnp.exp(masked - row_max[:, None]), 0.0)
            total = lax.optimization_barrier(jnp.sum(weights, axis=1))
            mixed = jnp.dot(weights.astype(jnp.bfloat16), head_values, preferred_element_type=jnp.float32)
            return ((mixed / total[:, None]).astype(jnp.bfloat16), jnp.max(row_max))
        per_head, head_max = lax.map(one_head, (jnp.transpose(query_nope, (1, 0, 2)), jnp.transpose(query_rope, (1, 0, 2)), jnp.transpose(key_nope, (1, 0, 2)), jnp.transpose(values, (1, 0, 2))))
        contexts.append(jnp.transpose(per_head, (1, 0, 2)).reshape(L, HEADS * VD))
        largest = jnp.maximum(largest, head_max)
    ratio = CLIP / jnp.maximum(largest, CLIP)
    root = jnp.sqrt(ratio)
    factors = jnp.concatenate([jnp.broadcast_to(root[:, None], (HEADS, NOPE)), jnp.broadcast_to(ratio[:, None], (HEADS, ROPE))], axis=1).reshape(HEADS * (NOPE + ROPE))
    clipped_uq = (w_uq.astype(jnp.float32) * factors[None, :]).astype(jnp.bfloat16)
    clipped_uk = (w_uk.astype(jnp.float32) * jnp.repeat(root, NOPE)[None, :]).astype(jnp.bfloat16)
    return (jnp.stack(contexts), clipped_uq, clipped_uk)
```

```python
import functools
import math

import jax
import jax.numpy as jnp
from jax import lax
from jax.experimental import pallas as pl
from jax.experimental.pallas import tpu as pltpu
from jax.sharding import PartitionSpec as P

NOPE = 128
ROPE = 64
VD = 128
CLIP = 8


rope_base = 50000.0
masked_value = -1e30


def turning(positions, width):
    steps = jnp.arange(width // 2, dtype=jnp.float32) * (2.0 / width)
    freqs = jnp.exp(-math.log(rope_base) * steps)
    angle = positions.astype(jnp.float32)[:, None] * freqs[None, :]
    return (jnp.cos(angle), jnp.sin(angle))


def rotate(values, cosine, sine):
    half = values.shape[-1] // 2
    first = values[..., :half]
    second = values[..., half:]
    return jnp.concatenate(
        [first * cosine - second * sine, second * cosine + first * sine], axis=-1
    )


def positions_of(index, order, half_block):
    which = index // half_block
    onehot = which[:, None] == jnp.arange(order.shape[0], dtype=jnp.int32)[None, :]
    base = jnp.sum(jnp.where(onehot, order[None, :], 0), axis=1)
    return base * half_block + index % half_block


def by_tokens(query_latent, key_latent, rope_key, w_uq, w_uk, w_uv, block_order, segment_ids):
    query_local, key_local = (
        lax.all_gather(query_latent[0], "tp", axis=1, tiled=True),
        lax.all_gather(key_latent[0], "tp", axis=1, tiled=True),
    )
    rows_uq, rows_uk, rows_uv = (
        lax.all_gather(w_uq, "seq", axis=0, tiled=True),
        lax.all_gather(w_uk, "seq", axis=0, tiled=True),
        lax.all_gather(w_uv, "seq", axis=0, tiled=True),
    )
    tok_rows = query_local.shape[0]
    half_block = tok_rows // 2
    order = block_order[0]
    labels_all = segment_ids[0]
    heads = w_uq.shape[1] // (NOPE + ROPE)
    scale = 1.0 / math.sqrt(NOPE + ROPE)
    own_index = lax.axis_index("seq") * tok_rows + jnp.arange(tok_rows, dtype=jnp.int32)
    query_pos = positions_of(own_index, order, half_block)
    query_labels = jnp.take(labels_all, query_pos)
    cosine, sine = turning(query_pos, ROPE)
    query_full = jnp.dot(query_local, rows_uq, preferred_element_type=jnp.float32).reshape(
        tok_rows, heads, NOPE + ROPE
    )
    query_nope = jnp.transpose(query_full[:, :, :NOPE].astype(jnp.bfloat16), (1, 0, 2))
    query_rope = jnp.transpose(
        rotate(query_full[:, :, NOPE:], cosine[:, None, :], sine[:, None, :]).astype(jnp.bfloat16),
        (1, 0, 2),
    )
    key_rope = rotate(rope_key[0].astype(jnp.float32), cosine, sine).astype(jnp.bfloat16)

    def slice_latent(pieces, first, width):
        latent_block = lax.dynamic_slice_in_dim(pieces[0], first, width, 0)
        rope_block = lax.dynamic_slice_in_dim(pieces[1], first, width, 0)
        nope_block = jnp.dot(latent_block, rows_uk, preferred_element_type=jnp.float32).astype(
            jnp.bfloat16
        )
        value_block = jnp.dot(latent_block, rows_uv, preferred_element_type=jnp.float32).astype(
            jnp.bfloat16
        )
        return (nope_block, value_block, rope_block)

    initial = (
        jnp.full((heads, tok_rows), masked_value, jnp.float32),
        jnp.zeros((heads, tok_rows), jnp.float32),
        jnp.zeros((heads, tok_rows, VD), jnp.float32),
    )
    pieces = (
        lax.all_gather(key_local, "seq", axis=0, tiled=True),
        lax.all_gather(key_rope, "seq", axis=0, tiled=True),
    )
    count = pieces[-1].shape[0]
    width = math.gcd(count, 512)

    def block_step(state, number):
        first = number * width
        nope_block, value_block, rope_block = slice_latent(pieces, first, width)
        nope_block = nope_block.reshape(width, heads, NOPE)
        value_block = value_block.reshape(width, heads, VD)
        key_index = first + jnp.arange(width, dtype=jnp.int32)
        key_pos = positions_of(key_index, order, half_block)
        key_labels = jnp.take(labels_all, key_pos)
        allowed = (key_pos[None, :] <= query_pos[:, None]) & (
            key_labels[None, :] == query_labels[:, None]
        )
        scores = jnp.einsum(
            "hqd,khd->hqk", query_nope, nope_block, preferred_element_type=jnp.float32
        )
        scores = (
            scores
            + jnp.einsum("hqr,kr->hqk", query_rope, rope_block, preferred_element_type=jnp.float32)
        ) * scale
        masked = jnp.where(allowed[None], scores, masked_value)
        run_max, run_total, run_sum = state
        new_max = jnp.maximum(run_max, jnp.max(masked, axis=2))
        weights = jnp.where(allowed[None], jnp.exp(masked - new_max[:, :, None]), 0.0)
        shrink = jnp.exp(run_max - new_max)
        new_total = run_total * shrink + jnp.sum(weights, axis=2)
        mixed = jnp.einsum(
            "hqk,khv->hqv",
            weights.astype(jnp.bfloat16),
            value_block,
            preferred_element_type=jnp.float32,
        )
        new_sum = run_sum * shrink[:, :, None] + mixed
        return ((new_max, new_total, new_sum), None)

    result, unused = lax.scan(block_step, initial, jnp.arange(count // width, dtype=jnp.int32))
    run_max, run_total, run_sum = result
    context = (run_sum / run_total[:, :, None]).astype(jnp.bfloat16)
    context = jnp.transpose(context, (1, 0, 2)).reshape(1, tok_rows, heads * VD)
    head_max = lax.pmax(jnp.max(run_max, axis=1), ("seq", "dp"))
    ratio = CLIP / jnp.maximum(head_max, CLIP)
    root = jnp.sqrt(ratio)
    factors = jnp.concatenate(
        [
            jnp.broadcast_to(root[:, None], (heads, NOPE)),
            jnp.broadcast_to(ratio[:, None], (heads, ROPE)),
        ],
        axis=1,
    ).reshape(heads * (NOPE + ROPE))
    clipped_uq = (w_uq.astype(jnp.float32) * factors[None, :]).astype(jnp.bfloat16)
    clipped_uk = (w_uk.astype(jnp.float32) * jnp.repeat(root, NOPE)[None, :]).astype(jnp.bfloat16)
    return (context, clipped_uq, clipped_uk)


def turned(values, cosine, sine):
    half = values.shape[-1] // 2
    swapped = jnp.concatenate([values[:, half:], values[:, :half]], axis=1)
    return values * cosine + swapped * sine


def attend(
    block, tile, own, order, first_chunk, stored_at,
    query_ref, key_ref, rope_ref, wq_ref, wk_ref, wv_ref, cos_ref, sin_ref, col_ref, row_ref,
    context_ref, peak_ref,
    q_s, k_s, v_s, s_s, m_s,
):
    count = query_ref.shape[0]
    scale = 1.0 / math.sqrt(NOPE + ROPE)
    width = NOPE + ROPE
    rows = min(count, 4 * block)

    def project(step, unused):
        at = pl.multiple_of(step * rows, rows)
        latent = key_ref[pl.ds(at, rows), :]
        nope = jnp.dot(latent, wk_ref[...], preferred_element_type=jnp.float32).astype(jnp.bfloat16)
        value = jnp.dot(latent, wv_ref[...], preferred_element_type=jnp.float32).astype(jnp.bfloat16)
        full = jnp.dot(
            query_ref[pl.ds(at, rows), :], wq_ref[...], preferred_element_type=jnp.float32
        )
        for part in range(rows // block):
            lo, hi = part * block, (part + 1) * block
            to = pl.multiple_of(order[step * (rows // block) + part] * block, block)
            there = pl.ds(to, block)
            cosine, sine = cos_ref[there, :], sin_ref[there, :]
            raw = rope_ref[pl.ds(pl.multiple_of(at + lo, block), block), :].astype(jnp.float32)
            key_rope = turned(raw, cosine, sine).astype(jnp.bfloat16)
            v_s[there, :] = value[lo:hi, :]
            for head in range(own):
                base = head * width
                k_s[head, there, :NOPE] = nope[lo:hi, head * NOPE : (head + 1) * NOPE]
                k_s[head, there, NOPE:] = key_rope
                q_s[head, there, :NOPE] = full[lo:hi, base : base + NOPE].astype(jnp.bfloat16)
                q_s[head, there, NOPE:] = turned(
                    full[lo:hi, base + NOPE : base + width], cosine, sine
                ).astype(jnp.bfloat16)
        return unused

    lax.fori_loop(0, count // rows, project, 0)

    def per_tile(number, best):
        first = first_chunk[number]
        here = pl.ds(pl.multiple_of(number * tile, tile), tile)
        for head in range(own):
            m_s[head] = jnp.full((tile, 128), masked_value, jnp.float32)

        def score(chunk, unused):
            there = pl.ds(pl.multiple_of(chunk * tile, tile), tile)
            gap = (chunk - number) * tile
            later = lax.broadcasted_iota(jnp.int32, (tile, tile), 1) + gap
            now = lax.broadcasted_iota(jnp.int32, (tile, tile), 0)
            allowed = (later <= now) & (col_ref[here, :] == row_ref[chunk])
            for head in range(own):
                raw = lax.dot_general(
                    q_s[head, here, :], k_s[head, there, :], (((1,), (1,)), ((), ())),
                    preferred_element_type=jnp.float32,
                )
                raw = jnp.where(allowed, raw, masked_value)
                s_s[chunk - first, head] = raw
                best_here = m_s[head]
                for lane in range(tile // 128):
                    best_here = jnp.maximum(best_here, raw[:, lane * 128 : (lane + 1) * 128])
                m_s[head] = best_here
            return unused

        lax.fori_loop(first, number + 1, score, 0)
        tops = []
        for head in range(own):
            top = jnp.max(m_s[head], axis=1, keepdims=True)
            m_s[head] = jnp.broadcast_to(top, (tile, 128))
            tops.append(jnp.broadcast_to(jnp.max(top, axis=0, keepdims=True), (1, 128)))

        factor = scale * math.log2(math.e)

        def mix(chunk, state):
            there = pl.ds(pl.multiple_of(chunk * tile, tile), tile)
            out = []
            for head in range(own):
                total, mixed = state[head]
                top = m_s[head]
                raw = s_s[chunk - first, head]
                pieces = [
                    jnp.exp2((raw[:, lane * 128 : (lane + 1) * 128] - top) * factor)
                    for lane in range(tile // 128)
                ]
                for piece in pieces:
                    total = total + piece
                weights = jnp.concatenate([piece.astype(jnp.bfloat16) for piece in pieces], axis=1)
                mixed = mixed + jnp.dot(
                    weights, v_s[there, head * VD : (head + 1) * VD],
                    preferred_element_type=jnp.float32,
                )
                out.append((total, mixed))
            return tuple(out)

        zero = tuple(
            (jnp.zeros((tile, 128), jnp.float32), jnp.zeros((tile, VD), jnp.float32))
            for head in range(own)
        )
        state = lax.fori_loop(first, number + 1, mix, zero)
        for head in range(own):
            total, mixed = state[head]
            done = (mixed / jnp.sum(total, axis=1, keepdims=True)).astype(jnp.bfloat16)
            for part in range(tile // block):
                to = pl.multiple_of(stored_at[number * (tile // block) + part] * block, block)
                context_ref[pl.ds(to, block), head * VD : (head + 1) * VD] = done[
                    part * block : (part + 1) * block, :
                ]
        return jnp.maximum(best, jnp.concatenate(tops, axis=0))

    best = lax.fori_loop(
        0, count // tile, per_tile, jnp.full((own, 128), masked_value, jnp.float32)
    )
    peak_ref[...] = best * scale


def by_heads(query_latent, key_latent, rope_key, w_uq, w_uk, w_uv, block_order, segment_ids):
    devices = lax.axis_size("seq")
    heads = w_uq.shape[1] // (NOPE + ROPE)
    own = heads // devices
    swap = functools.partial(
        lax.all_to_all, axis_name="seq", split_axis=1, concat_axis=0, tiled=True
    )
    wq, wk, wv = swap(w_uq), swap(w_uk), swap(w_uv)

    def everywhere(latent):
        return lax.all_gather(
            lax.all_gather(latent, "tp", axis=1, tiled=True), "seq", axis=0, tiled=True
        )

    query, key = everywhere(query_latent[0]), everywhere(key_latent[0])
    rope = lax.all_gather(rope_key[0], "seq", axis=0, tiled=True)
    order, labels = block_order[0], segment_ids[0]
    count, blocks = labels.shape[0], order.shape[0]
    block = count // blocks
    tile = 2 * block
    chunks = count // tile
    cosine, sine = turning(jnp.arange(count, dtype=jnp.int32), ROPE)
    cosine = jnp.concatenate([cosine, cosine], axis=1)
    sine = jnp.concatenate([-sine, sine], axis=1)
    stored_at = jnp.argmax(
        order[None, :] == jnp.arange(blocks, dtype=jnp.int32)[:, None], axis=1
    ).astype(jnp.int32)
    heads_of = labels[::tile]
    first_chunk = (
        jnp.sum((labels[None, :] < heads_of[:, None]).astype(jnp.int32), axis=1) // tile
    ).astype(jnp.int32)
    vmem = pl.BlockSpec(memory_space=pltpu.VMEM)
    smem = pl.BlockSpec(memory_space=pltpu.SMEM)
    context, peak = pl.pallas_call(
        functools.partial(attend, block, tile, own),
        out_shape=(
            jax.ShapeDtypeStruct((count, own * VD), jnp.bfloat16),
            jax.ShapeDtypeStruct((own, 128), jnp.float32),
        ),
        in_specs=[smem] * 3 + [vmem] * 10,
        out_specs=(vmem, vmem),
        scratch_shapes=[
            pltpu.VMEM((own, count, NOPE + ROPE), jnp.bfloat16),
            pltpu.VMEM((own, count, NOPE + ROPE), jnp.bfloat16),
            pltpu.VMEM((count, own * VD), jnp.bfloat16),
            pltpu.VMEM((chunks, own, tile, tile), jnp.float32),
            pltpu.VMEM((own, tile, 128), jnp.float32),
        ],
        compiler_params=pltpu.CompilerParams(vmem_limit_bytes=60 * 1024 * 1024),
        cost_estimate=pl.CostEstimate(
            flops=12_000_000_000, bytes_accessed=16_000_000, transcendentals=4_000_000
        ),
        name="attend",
    )(
        order, first_chunk, stored_at, query, key, rope, wq, wk, wv, cosine, sine,
        labels[:, None], labels.reshape(chunks, 1, tile),
    )
    context = lax.all_to_all(context, "seq", split_axis=0, concat_axis=1, tiled=True)[None]
    mine = lax.dynamic_update_slice(
        jnp.full((heads,), masked_value, jnp.float32), peak[:, 0], (lax.axis_index("seq") * own,)
    )
    return (context,) + clipped(w_uq, w_uk, lax.pmax(mine, ("seq", "dp")), heads)


def clipped(w_uq, w_uk, head_max, heads):
    ratio = CLIP / jnp.maximum(head_max, CLIP)
    root = jnp.sqrt(ratio)
    factors = jnp.concatenate(
        [
            jnp.broadcast_to(root[:, None], (heads, NOPE)),
            jnp.broadcast_to(ratio[:, None], (heads, ROPE)),
        ],
        axis=1,
    ).reshape(heads * (NOPE + ROPE))
    clipped_uq = (w_uq.astype(jnp.float32) * factors[None, :]).astype(jnp.bfloat16)
    clipped_uk = (w_uk.astype(jnp.float32) * jnp.repeat(root, NOPE)[None, :]).astype(jnp.bfloat16)
    return (clipped_uq, clipped_uk)


def on_device(*arrays):
    heads = arrays[3].shape[1] // (NOPE + ROPE)
    if heads % (2 * lax.axis_size("seq")) == 0:
        return by_heads(*arrays)
    return by_tokens(*arrays)


def solution(mesh):
    placed = (
        P("dp", "seq", "tp"),
        P("dp", "seq", "tp"),
        P("dp", "seq", None),
        P("seq", "tp"),
        P("seq", "tp"),
        P("seq", "tp"),
        P("dp", None),
        P("dp", None),
    )
    return jax.shard_map(
        on_device,
        mesh=mesh,
        in_specs=placed,
        out_specs=(P("dp", "seq", "tp"), P("seq", "tp"), P("seq", "tp")),
        check_vma=False,
    )
```

```python
import functools
import math

import jax
import jax.numpy as jnp
from jax import lax
from jax.experimental import pallas as pl
from jax.experimental.pallas import tpu as pltpu
from jax.sharding import PartitionSpec as P

NOPE = 128
ROPE = 64
VD = 128
CLIP = 8


rope_base = 50000.0
masked_value = -1e30


def turning(positions, width):
    steps = jnp.arange(width // 2, dtype=jnp.float32) * (2.0 / width)
    freqs = jnp.exp(-math.log(rope_base) * steps)
    angle = positions.astype(jnp.float32)[:, None] * freqs[None, :]
    return (jnp.cos(angle), jnp.sin(angle))


def rotate(values, cosine, sine):
    half = values.shape[-1] // 2
    first = values[..., :half]
    second = values[..., half:]
    return jnp.concatenate(
        [first * cosine - second * sine, second * cosine + first * sine], axis=-1
    )


def positions_of(index, order, half_block):
    which = index // half_block
    onehot = which[:, None] == jnp.arange(order.shape[0], dtype=jnp.int32)[None, :]
    base = jnp.sum(jnp.where(onehot, order[None, :], 0), axis=1)
    return base * half_block + index % half_block


def by_tokens(query_latent, key_latent, rope_key, w_uq, w_uk, w_uv, block_order, segment_ids):
    query_local, key_local = (
        lax.all_gather(query_latent[0], "tp", axis=1, tiled=True),
        lax.all_gather(key_latent[0], "tp", axis=1, tiled=True),
    )
    rows_uq, rows_uk, rows_uv = (
        lax.all_gather(w_uq, "seq", axis=0, tiled=True),
        lax.all_gather(w_uk, "seq", axis=0, tiled=True),
        lax.all_gather(w_uv, "seq", axis=0, tiled=True),
    )
    tok_rows = query_local.shape[0]
    half_block = tok_rows // 2
    order = block_order[0]
    labels_all = segment_ids[0]
    heads = w_uq.shape[1] // (NOPE + ROPE)
    scale = 1.0 / math.sqrt(NOPE + ROPE)
    own_index = lax.axis_index("seq") * tok_rows + jnp.arange(tok_rows, dtype=jnp.int32)
    query_pos = positions_of(own_index, order, half_block)
    query_labels = jnp.take(labels_all, query_pos)
    cosine, sine = turning(query_pos, ROPE)
    query_full = jnp.dot(query_local, rows_uq, preferred_element_type=jnp.float32).reshape(
        tok_rows, heads, NOPE + ROPE
    )
    query_nope = jnp.transpose(query_full[:, :, :NOPE].astype(jnp.bfloat16), (1, 0, 2))
    query_rope = jnp.transpose(
        rotate(query_full[:, :, NOPE:], cosine[:, None, :], sine[:, None, :]).astype(jnp.bfloat16),
        (1, 0, 2),
    )
    key_rope = rotate(rope_key[0].astype(jnp.float32), cosine, sine).astype(jnp.bfloat16)

    def slice_latent(pieces, first, width):
        latent_block = lax.dynamic_slice_in_dim(pieces[0], first, width, 0)
        rope_block = lax.dynamic_slice_in_dim(pieces[1], first, width, 0)
        nope_block = jnp.dot(latent_block, rows_uk, preferred_element_type=jnp.float32).astype(
            jnp.bfloat16
        )
        value_block = jnp.dot(latent_block, rows_uv, preferred_element_type=jnp.float32).astype(
            jnp.bfloat16
        )
        return (nope_block, value_block, rope_block)

    initial = (
        jnp.full((heads, tok_rows), masked_value, jnp.float32),
        jnp.zeros((heads, tok_rows), jnp.float32),
        jnp.zeros((heads, tok_rows, VD), jnp.float32),
    )
    pieces = (
        lax.all_gather(key_local, "seq", axis=0, tiled=True),
        lax.all_gather(key_rope, "seq", axis=0, tiled=True),
    )
    count = pieces[-1].shape[0]
    width = math.gcd(count, 512)

    def block_step(state, number):
        first = number * width
        nope_block, value_block, rope_block = slice_latent(pieces, first, width)
        nope_block = nope_block.reshape(width, heads, NOPE)
        value_block = value_block.reshape(width, heads, VD)
        key_index = first + jnp.arange(width, dtype=jnp.int32)
        key_pos = positions_of(key_index, order, half_block)
        key_labels = jnp.take(labels_all, key_pos)
        allowed = (key_pos[None, :] <= query_pos[:, None]) & (
            key_labels[None, :] == query_labels[:, None]
        )
        scores = jnp.einsum(
            "hqd,khd->hqk", query_nope, nope_block, preferred_element_type=jnp.float32
        )
        scores = (
            scores
            + jnp.einsum("hqr,kr->hqk", query_rope, rope_block, preferred_element_type=jnp.float32)
        ) * scale
        masked = jnp.where(allowed[None], scores, masked_value)
        run_max, run_total, run_sum = state
        new_max = jnp.maximum(run_max, jnp.max(masked, axis=2))
        weights = jnp.where(allowed[None], jnp.exp(masked - new_max[:, :, None]), 0.0)
        shrink = jnp.exp(run_max - new_max)
        new_total = run_total * shrink + jnp.sum(weights, axis=2)
        mixed = jnp.einsum(
            "hqk,khv->hqv",
            weights.astype(jnp.bfloat16),
            value_block,
            preferred_element_type=jnp.float32,
        )
        new_sum = run_sum * shrink[:, :, None] + mixed
        return ((new_max, new_total, new_sum), None)

    result, unused = lax.scan(block_step, initial, jnp.arange(count // width, dtype=jnp.int32))
    run_max, run_total, run_sum = result
    context = (run_sum / run_total[:, :, None]).astype(jnp.bfloat16)
    context = jnp.transpose(context, (1, 0, 2)).reshape(1, tok_rows, heads * VD)
    head_max = lax.pmax(jnp.max(run_max, axis=1), ("seq", "dp"))
    ratio = CLIP / jnp.maximum(head_max, CLIP)
    root = jnp.sqrt(ratio)
    factors = jnp.concatenate(
        [
            jnp.broadcast_to(root[:, None], (heads, NOPE)),
            jnp.broadcast_to(ratio[:, None], (heads, ROPE)),
        ],
        axis=1,
    ).reshape(heads * (NOPE + ROPE))
    clipped_uq = (w_uq.astype(jnp.float32) * factors[None, :]).astype(jnp.bfloat16)
    clipped_uk = (w_uk.astype(jnp.float32) * jnp.repeat(root, NOPE)[None, :]).astype(jnp.bfloat16)
    return (context, clipped_uq, clipped_uk)


def turned(values, cosine, sine):
    half = values.shape[-1] // 2
    swapped = jnp.concatenate([values[:, half:], values[:, :half]], axis=1)
    return values * cosine + swapped * sine


def attend(
    block, tile, own, order, first_chunk, stored_at,
    query_ref, key_ref, rope_ref, wq_ref, wk_ref, wv_ref, cos_ref, sin_ref, col_ref, row_ref,
    context_ref, peak_ref,
    q_s, k_s, v_s, s_s, m_s,
):
    count = query_ref.shape[0]
    scale = 1.0 / math.sqrt(NOPE + ROPE)
    width = NOPE + ROPE
    rows = min(count, 4 * block)

    def project(step, unused):
        at = pl.multiple_of(step * rows, rows)
        latent = key_ref[pl.ds(at, rows), :]
        nope = jnp.dot(latent, wk_ref[...], preferred_element_type=jnp.float32).astype(jnp.bfloat16)
        value = jnp.dot(latent, wv_ref[...], preferred_element_type=jnp.float32).astype(jnp.bfloat16)
        full = jnp.dot(
            query_ref[pl.ds(at, rows), :], wq_ref[...], preferred_element_type=jnp.float32
        )
        for part in range(rows // block):
            lo, hi = part * block, (part + 1) * block
            to = pl.multiple_of(order[step * (rows // block) + part] * block, block)
            there = pl.ds(to, block)
            cosine, sine = cos_ref[there, :], sin_ref[there, :]
            raw = rope_ref[pl.ds(pl.multiple_of(at + lo, block), block), :].astype(jnp.float32)
            key_rope = turned(raw, cosine, sine).astype(jnp.bfloat16)
            v_s[there, :] = value[lo:hi, :]
            for head in range(own):
                base = head * width
                k_s[head, there, :NOPE] = nope[lo:hi, head * NOPE : (head + 1) * NOPE]
                k_s[head, there, NOPE:] = key_rope
                q_s[head, there, :NOPE] = full[lo:hi, base : base + NOPE].astype(jnp.bfloat16)
                q_s[head, there, NOPE:] = turned(
                    full[lo:hi, base + NOPE : base + width], cosine, sine
                ).astype(jnp.bfloat16)
        return unused

    lax.fori_loop(0, count // rows, project, 0)

    def per_tile(number, best):
        first = first_chunk[number]
        here = pl.ds(pl.multiple_of(number * tile, tile), tile)
        for head in range(own):
            m_s[head] = jnp.full((tile, 128), masked_value, jnp.float32)

        def score(chunk, unused):
            there = pl.ds(pl.multiple_of(chunk * tile, tile), tile)
            gap = (chunk - number) * tile
            later = lax.broadcasted_iota(jnp.int32, (tile, tile), 1) + gap
            now = lax.broadcasted_iota(jnp.int32, (tile, tile), 0)
            allowed = (later <= now) & (col_ref[here, :] == row_ref[chunk])
            for head in range(own):
                raw = lax.dot_general(
                    q_s[head, here, :], k_s[head, there, :], (((1,), (1,)), ((), ())),
                    preferred_element_type=jnp.float32,
                )
                raw = jnp.where(allowed, raw, masked_value)
                s_s[chunk - first, head] = raw
                best_here = m_s[head]
                for lane in range(tile // 128):
                    best_here = jnp.maximum(best_here, raw[:, lane * 128 : (lane + 1) * 128])
                m_s[head] = best_here
            return unused

        lax.fori_loop(first, number + 1, score, 0)
        tops = []
        for head in range(own):
            top = jnp.max(m_s[head], axis=1, keepdims=True)
            m_s[head] = jnp.broadcast_to(top, (tile, 128))
            tops.append(jnp.broadcast_to(jnp.max(top, axis=0, keepdims=True), (1, 128)))

        factor = scale * math.log2(math.e)

        def mix(chunk, state):
            there = pl.ds(pl.multiple_of(chunk * tile, tile), tile)
            out = []
            for head in range(own):
                total, mixed = state[head]
                top = m_s[head]
                raw = s_s[chunk - first, head]
                pieces = [
                    jnp.exp2((raw[:, lane * 128 : (lane + 1) * 128] - top) * factor)
                    for lane in range(tile // 128)
                ]
                for piece in pieces:
                    total = total + piece
                weights = jnp.concatenate([piece.astype(jnp.bfloat16) for piece in pieces], axis=1)
                mixed = mixed + jnp.dot(
                    weights, v_s[there, head * VD : (head + 1) * VD],
                    preferred_element_type=jnp.float32,
                )
                out.append((total, mixed))
            return tuple(out)

        zero = tuple(
            (jnp.zeros((tile, 128), jnp.float32), jnp.zeros((tile, VD), jnp.float32))
            for head in range(own)
        )
        state = lax.fori_loop(first, number + 1, mix, zero)
        for head in range(own):
            total, mixed = state[head]
            done = (mixed / jnp.sum(total, axis=1, keepdims=True)).astype(jnp.bfloat16)
            for part in range(tile // block):
                to = pl.multiple_of(stored_at[number * (tile // block) + part] * block, block)
                context_ref[pl.ds(to, block), head * VD : (head + 1) * VD] = done[
                    part * block : (part + 1) * block, :
                ]
        return jnp.maximum(best, jnp.concatenate(tops, axis=0))

    best = lax.fori_loop(
        0, count // tile, per_tile, jnp.full((own, 128), masked_value, jnp.float32)
    )
    peak_ref[...] = best * scale


MESH = pl.DeviceIdType.MESH


def window(start, size):
    return pl.ds(pl.multiple_of(start * size, size), size)


def greet(wheres):
    barrier = pltpu.get_barrier_semaphore()
    for where in wheres:
        pl.semaphore_signal(barrier, inc=1, device_id=where, device_id_type=MESH)
    pl.semaphore_wait(barrier, len(wheres))


def spread(
    n, query_ref, key_ref, rope_ref, uq_ref, uk_ref, uv_ref,
    query_out, key_out, rope_out, wq_out, wk_out, wv_out,
    sends, got_query, got_key, got_rope, got_weight, local,
):
    s, t, d = lax.axis_index("seq"), lax.axis_index("tp"), lax.axis_index("dp")
    partner = s + 1 - 2 * lax.rem(s, 2)
    near = sorted(range(1, n // 2), key=lambda k: (min(k, n // 2 - k), k))
    same = lambda k: lax.rem(s + 2 * k, n)
    cross = lambda k: lax.rem(partner + 2 * k, n)
    beside, across, mate = {"tp": 1 - t}, {"dp": 1 - d}, {"seq": partner}
    greet(
        [mate, beside, across]
        + [{"seq": same(k)} for k in near]
        + [{"seq": cross(k)} for k in near]
    )
    rows, wide = query_ref.shape
    thin = key_ref.shape[1]
    weights = ((uq_ref, wq_out), (uk_ref, wk_out), (uv_ref, wv_out))
    started = []

    def link(source, target, arrived, where, sender):
        return pltpu.make_async_remote_copy(
            src_ref=source, dst_ref=target, send_sem=sends.at[sender], recv_sem=arrived,
            device_id=where, device_id_type=MESH,
        )

    def send(source, target, arrived, where):
        copy = link(source, target, arrived, where, len(started))
        copy.start()
        started.append(copy)

    def arrive(target, arrived):
        link(target, target, arrived, mate, 0).wait_recv()

    def spots(src, tp):
        return (
            (query_out.at[window(src, rows), window(tp, wide)], got_query.at[src, tp]),
            (key_out.at[window(src, rows), window(tp, thin)], got_key.at[src, tp]),
        )

    def rope_spot(src):
        return (rope_out.at[window(src, rows), :], got_rope.at[src])

    def own_latents(where, rope):
        for source, (target, arrived) in zip((query_ref, key_ref), spots(s, t)):
            send(source, target, arrived, where)
        if rope:
            send(rope_ref, *rope_spot(s), where)

    def await_latents(src, tp, rope):
        for target, arrived in spots(src, tp):
            arrive(target, arrived)
        if rope:
            arrive(*rope_spot(src))

    def pass_latents(src, tp, where, rope):
        for target, arrived in spots(src, tp):
            send(target, target, arrived, where)
        if rope:
            target, arrived = rope_spot(src)
            send(target, target, arrived, where)

    def weight_spot(index, src, half):
        out = weights[index][1]
        depth = weights[index][0].shape[0] // 2
        return (out.at[window(src * 2 + half, depth), :], got_weight.at[index, src, half])

    def own_weights(to):
        for index, (ref, out) in enumerate(weights):
            piece = ref.at[window(d, ref.shape[0] // 2), window(to, out.shape[1])]
            send(piece, *weight_spot(index, s, d), {"seq": to})

    def pass_weights(src):
        for index in range(len(weights)):
            target, arrived = weight_spot(index, src, d)
            arrive(target, arrived)
            send(target, target, arrived, across)

    own_latents(beside, False)
    for k in near:
        own_latents({"seq": same(k)}, True)
        own_weights(same(k))
        own_weights(cross(k))
    own_latents(mate, True)
    own_weights(partner)
    kept = [
        pltpu.make_async_copy(source, target, local.at[place])
        for place, (source, target) in enumerate(
            [(query_ref, spots(s, t)[0][0]), (key_ref, spots(s, t)[1][0]), (rope_ref, rope_spot(s)[0])]
            + [
                (ref.at[:, window(s, out.shape[1])], out.at[window(s, ref.shape[0]), :])
                for ref, out in weights
            ]
        )
    ]
    for copy in kept:
        copy.start()
    pass_weights(partner)
    for k in near:
        await_latents(same(k), t, True)
        pass_latents(same(k), t, beside, False)
        pass_latents(same(k), t, mate, True)
        pass_weights(same(k))
        pass_weights(cross(k))
    for k in [0] + near:
        await_latents(same(k), 1 - t, False)
        pass_latents(same(k), 1 - t, mate, False)
    for k in [0] + near:
        await_latents(cross(k), t, True)
        await_latents(cross(k), 1 - t, False)
    for src in [partner] + [same(k) for k in near] + [cross(k) for k in near]:
        for index in range(len(weights)):
            arrive(*weight_spot(index, src, 1 - d))
    for copy in started:
        copy.wait_send()
    for copy in kept:
        copy.wait()


def give_back(n, context_ref, peak_ref, out_ref, peaks_ref, sends, got_context, got_peak, local):
    s, d = lax.axis_index("seq"), lax.axis_index("dp")
    rows, wide = out_ref.shape[0], context_ref.shape[1]
    steps = [k for k in range(1, n)]
    peers = [lax.rem(s + k, n) for k in steps]
    wheres = [{"seq": to} for to in peers]
    others = [{"dp": 1 - d}] + [{"seq": to, "dp": 1 - d} for to in peers]
    greet(wheres + others)
    started = []

    def link(source, target, arrived, where, sender):
        return pltpu.make_async_remote_copy(
            src_ref=source, dst_ref=target, send_sem=sends.at[sender], recv_sem=arrived,
            device_id=where, device_id_type=MESH,
        )

    def send(source, target, arrived, where):
        copy = link(source, target, arrived, where, len(started))
        copy.start()
        started.append(copy)

    me = d * n + s
    for where in wheres + others:
        send(peak_ref, peaks_ref.at[me], got_peak.at[me], where)
    for to, where in zip(peers, wheres):
        send(context_ref.at[window(to, rows), :], out_ref.at[:, window(s, wide)], got_context.at[s], where)
    kept = [
        pltpu.make_async_copy(peak_ref, peaks_ref.at[me], local.at[0]),
        pltpu.make_async_copy(context_ref.at[window(s, rows), :], out_ref.at[:, window(s, wide)], local.at[1]),
    ]
    for copy in kept:
        copy.start()
    for src in peers:
        target = out_ref.at[:, window(src, wide)]
        link(target, target, got_context.at[src], wheres[0], 0).wait_recv()
    for src in [d * n + p for p in peers] + [(1 - d) * n + p for p in peers] + [(1 - d) * n + s]:
        link(peaks_ref.at[src], peaks_ref.at[src], got_peak.at[src], wheres[0], 0).wait_recv()
    for copy in started:
        copy.wait_send()
    for copy in kept:
        copy.wait()


def by_heads(query_latent, key_latent, rope_key, w_uq, w_uk, w_uv, block_order, segment_ids):
    devices = lax.axis_size("seq")
    heads = w_uq.shape[1] // (NOPE + ROPE)
    own = heads // devices
    anyplace = pl.BlockSpec(memory_space=pl.ANY)
    vmem = pl.BlockSpec(memory_space=pltpu.VMEM)
    smem = pl.BlockSpec(memory_space=pltpu.SMEM)
    sides = lax.axis_size("tp")
    rows = query_latent.shape[1]
    shapes = (
        (devices * rows, sides * query_latent.shape[2]),
        (devices * rows, sides * key_latent.shape[2]),
        (devices * rows, ROPE),
        (devices * w_uq.shape[0], w_uq.shape[1] // devices),
        (devices * w_uk.shape[0], w_uk.shape[1] // devices),
        (devices * w_uv.shape[0], w_uv.shape[1] // devices),
    )
    half = devices // 2
    copies = 10 * half + 6 * (half - 1) + 3 * half + 6 * (devices - 1)
    query, key, rope, wq, wk, wv = pl.pallas_call(
        functools.partial(spread, devices),
        out_shape=[jax.ShapeDtypeStruct(shape, jnp.bfloat16) for shape in shapes],
        in_specs=[anyplace] * 6,
        out_specs=[anyplace] * 6,
        scratch_shapes=[
            pltpu.SemaphoreType.DMA((copies,)),
            pltpu.SemaphoreType.DMA((devices, sides)),
            pltpu.SemaphoreType.DMA((devices, sides)),
            pltpu.SemaphoreType.DMA((devices,)),
            pltpu.SemaphoreType.DMA((3, devices, 2)),
            pltpu.SemaphoreType.DMA((6,)),
        ],
        compiler_params=pltpu.CompilerParams(collective_id=0, has_side_effects=True),
        cost_estimate=pl.CostEstimate(
            flops=30_000_000_000, bytes_accessed=16_000_000, transcendentals=0
        ),
        name="spread",
    )(query_latent[0], key_latent[0], rope_key[0], w_uq, w_uk, w_uv)
    order, labels = block_order[0], segment_ids[0]
    count, blocks = labels.shape[0], order.shape[0]
    block = count // blocks
    tile = 2 * block
    chunks = count // tile
    cosine, sine = turning(jnp.arange(count, dtype=jnp.int32), ROPE)
    cosine = jnp.concatenate([cosine, cosine], axis=1)
    sine = jnp.concatenate([-sine, sine], axis=1)
    stored_at = jnp.argmax(
        order[None, :] == jnp.arange(blocks, dtype=jnp.int32)[:, None], axis=1
    ).astype(jnp.int32)
    heads_of = labels[::tile]
    first_chunk = (
        jnp.sum((labels[None, :] < heads_of[:, None]).astype(jnp.int32), axis=1) // tile
    ).astype(jnp.int32)
    context, peak = pl.pallas_call(
        functools.partial(attend, block, tile, own),
        out_shape=(
            jax.ShapeDtypeStruct((count, own * VD), jnp.bfloat16),
            jax.ShapeDtypeStruct((own, 128), jnp.float32),
        ),
        in_specs=[smem] * 3 + [vmem] * 10,
        out_specs=(vmem, vmem),
        scratch_shapes=[
            pltpu.VMEM((own, count, NOPE + ROPE), jnp.bfloat16),
            pltpu.VMEM((own, count, NOPE + ROPE), jnp.bfloat16),
            pltpu.VMEM((count, own * VD), jnp.bfloat16),
            pltpu.VMEM((chunks, own, tile, tile), jnp.float32),
            pltpu.VMEM((own, tile, 128), jnp.float32),
        ],
        compiler_params=pltpu.CompilerParams(vmem_limit_bytes=60 * 1024 * 1024),
        cost_estimate=pl.CostEstimate(
            flops=12_000_000_000, bytes_accessed=16_000_000, transcendentals=4_000_000
        ),
        name="attend",
    )(
        order, first_chunk, stored_at, query, key, rope, wq, wk, wv, cosine, sine,
        labels[:, None], labels.reshape(chunks, 1, tile),
    )
    context, peaks = pl.pallas_call(
        functools.partial(give_back, devices),
        out_shape=[
            jax.ShapeDtypeStruct((rows, heads * VD), jnp.bfloat16),
            jax.ShapeDtypeStruct((2 * devices, own, 128), jnp.float32),
        ],
        in_specs=[anyplace, vmem],
        out_specs=[anyplace, vmem],
        scratch_shapes=[
            pltpu.SemaphoreType.DMA((3 * devices,)),
            pltpu.SemaphoreType.DMA((devices,)),
            pltpu.SemaphoreType.DMA((2 * devices,)),
            pltpu.SemaphoreType.DMA((2,)),
        ],
        compiler_params=pltpu.CompilerParams(collective_id=1, has_side_effects=True),
        name="give_back",
    )(context, peak)
    head_max = jnp.max(peaks[:, :, 0].reshape(2, heads), axis=0)
    return (context[None],) + clipped(w_uq, w_uk, head_max, heads)


def clipped(w_uq, w_uk, head_max, heads):
    ratio = CLIP / jnp.maximum(head_max, CLIP)
    root = jnp.sqrt(ratio)
    factors = jnp.concatenate(
        [
            jnp.broadcast_to(root[:, None], (heads, NOPE)),
            jnp.broadcast_to(ratio[:, None], (heads, ROPE)),
        ],
        axis=1,
    ).reshape(heads * (NOPE + ROPE))
    clipped_uq = (w_uq.astype(jnp.float32) * factors[None, :]).astype(jnp.bfloat16)
    clipped_uk = (w_uk.astype(jnp.float32) * jnp.repeat(root, NOPE)[None, :]).astype(jnp.bfloat16)
    return (clipped_uq, clipped_uk)


def on_device(*arrays):
    heads = arrays[3].shape[1] // (NOPE + ROPE)
    pairs = lax.axis_size("tp") == 2 and lax.axis_size("dp") == 2
    if pairs and heads % (2 * lax.axis_size("seq")) == 0:
        return by_heads(*arrays)
    return by_tokens(*arrays)


def solution(mesh):
    placed = (
        P("dp", "seq", "tp"),
        P("dp", "seq", "tp"),
        P("dp", "seq", None),
        P("seq", "tp"),
        P("seq", "tp"),
        P("seq", "tp"),
        P("dp", None),
        P("dp", None),
    )
    return jax.shard_map(
        on_device,
        mesh=mesh,
        in_specs=placed,
        out_specs=(P("dp", "seq", "tp"), P("seq", "tp"), P("seq", "tp")),
        check_vma=False,
    )
```

```python
import functools
import math

import jax
import jax.numpy as jnp
import numpy as np
from jax import lax
from jax.experimental import pallas as pl
from jax.experimental.pallas import tpu as pltpu
from jax.sharding import PartitionSpec as P

NOPE = 128
ROPE = 64
VD = 128
CLIP = 8


rope_base = 50000.0
masked_value = -1e30


def turning(positions, width):
    steps = jnp.arange(width // 2, dtype=jnp.float32) * (2.0 / width)
    freqs = jnp.exp(-math.log(rope_base) * steps)
    angle = positions.astype(jnp.float32)[:, None] * freqs[None, :]
    return (jnp.cos(angle), jnp.sin(angle))


def rotate(values, cosine, sine):
    half = values.shape[-1] // 2
    first = values[..., :half]
    second = values[..., half:]
    return jnp.concatenate(
        [first * cosine - second * sine, second * cosine + first * sine], axis=-1
    )


def positions_of(index, order, half_block):
    which = index // half_block
    onehot = which[:, None] == jnp.arange(order.shape[0], dtype=jnp.int32)[None, :]
    base = jnp.sum(jnp.where(onehot, order[None, :], 0), axis=1)
    return base * half_block + index % half_block


def by_tokens(query_latent, key_latent, rope_key, w_uq, w_uk, w_uv, block_order, segment_ids):
    query_local, key_local = (
        lax.all_gather(query_latent[0], "tp", axis=1, tiled=True),
        lax.all_gather(key_latent[0], "tp", axis=1, tiled=True),
    )
    rows_uq, rows_uk, rows_uv = (
        lax.all_gather(w_uq, "seq", axis=0, tiled=True),
        lax.all_gather(w_uk, "seq", axis=0, tiled=True),
        lax.all_gather(w_uv, "seq", axis=0, tiled=True),
    )
    tok_rows = query_local.shape[0]
    half_block = tok_rows // 2
    order = block_order[0]
    labels_all = segment_ids[0]
    heads = w_uq.shape[1] // (NOPE + ROPE)
    scale = 1.0 / math.sqrt(NOPE + ROPE)
    own_index = lax.axis_index("seq") * tok_rows + jnp.arange(tok_rows, dtype=jnp.int32)
    query_pos = positions_of(own_index, order, half_block)
    query_labels = jnp.take(labels_all, query_pos)
    cosine, sine = turning(query_pos, ROPE)
    query_full = jnp.dot(query_local, rows_uq, preferred_element_type=jnp.float32).reshape(
        tok_rows, heads, NOPE + ROPE
    )
    query_nope = jnp.transpose(query_full[:, :, :NOPE].astype(jnp.bfloat16), (1, 0, 2))
    query_rope = jnp.transpose(
        rotate(query_full[:, :, NOPE:], cosine[:, None, :], sine[:, None, :]).astype(jnp.bfloat16),
        (1, 0, 2),
    )
    key_rope = rotate(rope_key[0].astype(jnp.float32), cosine, sine).astype(jnp.bfloat16)

    def slice_latent(pieces, first, width):
        latent_block = lax.dynamic_slice_in_dim(pieces[0], first, width, 0)
        rope_block = lax.dynamic_slice_in_dim(pieces[1], first, width, 0)
        nope_block = jnp.dot(latent_block, rows_uk, preferred_element_type=jnp.float32).astype(
            jnp.bfloat16
        )
        value_block = jnp.dot(latent_block, rows_uv, preferred_element_type=jnp.float32).astype(
            jnp.bfloat16
        )
        return (nope_block, value_block, rope_block)

    initial = (
        jnp.full((heads, tok_rows), masked_value, jnp.float32),
        jnp.zeros((heads, tok_rows), jnp.float32),
        jnp.zeros((heads, tok_rows, VD), jnp.float32),
    )
    pieces = (
        lax.all_gather(key_local, "seq", axis=0, tiled=True),
        lax.all_gather(key_rope, "seq", axis=0, tiled=True),
    )
    count = pieces[-1].shape[0]
    width = math.gcd(count, 512)

    def block_step(state, number):
        first = number * width
        nope_block, value_block, rope_block = slice_latent(pieces, first, width)
        nope_block = nope_block.reshape(width, heads, NOPE)
        value_block = value_block.reshape(width, heads, VD)
        key_index = first + jnp.arange(width, dtype=jnp.int32)
        key_pos = positions_of(key_index, order, half_block)
        key_labels = jnp.take(labels_all, key_pos)
        allowed = (key_pos[None, :] <= query_pos[:, None]) & (
            key_labels[None, :] == query_labels[:, None]
        )
        scores = jnp.einsum(
            "hqd,khd->hqk", query_nope, nope_block, preferred_element_type=jnp.float32
        )
        scores = (
            scores
            + jnp.einsum("hqr,kr->hqk", query_rope, rope_block, preferred_element_type=jnp.float32)
        ) * scale
        masked = jnp.where(allowed[None], scores, masked_value)
        run_max, run_total, run_sum = state
        new_max = jnp.maximum(run_max, jnp.max(masked, axis=2))
        weights = jnp.where(allowed[None], jnp.exp(masked - new_max[:, :, None]), 0.0)
        shrink = jnp.exp(run_max - new_max)
        new_total = run_total * shrink + jnp.sum(weights, axis=2)
        mixed = jnp.einsum(
            "hqk,khv->hqv",
            weights.astype(jnp.bfloat16),
            value_block,
            preferred_element_type=jnp.float32,
        )
        new_sum = run_sum * shrink[:, :, None] + mixed
        return ((new_max, new_total, new_sum), None)

    result, unused = lax.scan(block_step, initial, jnp.arange(count // width, dtype=jnp.int32))
    run_max, run_total, run_sum = result
    context = (run_sum / run_total[:, :, None]).astype(jnp.bfloat16)
    context = jnp.transpose(context, (1, 0, 2)).reshape(1, tok_rows, heads * VD)
    head_max = lax.pmax(jnp.max(run_max, axis=1), ("seq", "dp"))
    ratio = CLIP / jnp.maximum(head_max, CLIP)
    root = jnp.sqrt(ratio)
    factors = jnp.concatenate(
        [
            jnp.broadcast_to(root[:, None], (heads, NOPE)),
            jnp.broadcast_to(ratio[:, None], (heads, ROPE)),
        ],
        axis=1,
    ).reshape(heads * (NOPE + ROPE))
    clipped_uq = (w_uq.astype(jnp.float32) * factors[None, :]).astype(jnp.bfloat16)
    clipped_uk = (w_uk.astype(jnp.float32) * jnp.repeat(root, NOPE)[None, :]).astype(jnp.bfloat16)
    return (context, clipped_uq, clipped_uk)


def turned(values, cosine, sine):
    half = values.shape[-1] // 2
    swapped = jnp.concatenate([values[:, half:], values[:, :half]], axis=1)
    return values * cosine + swapped * sine


def attend(
    block, tile, own, order, labels,
    query_ref, key_ref, rope_ref, wq_ref, wk_ref, wv_ref, turn_ref, row_ref,
    context_ref, peak_ref,
    q_s, k_s, v_s, s_s, m_s, stored_at,
):
    count = query_ref.shape[0]
    scale = 1.0 / math.sqrt(NOPE + ROPE)
    width = NOPE + ROPE
    rows = min(count, 4 * block)
    for stored in range(count // block):
        stored_at[order[stored]] = stored

    def project(step, unused):
        at = pl.multiple_of(step * rows, rows)
        latent = key_ref[pl.ds(at, rows), :]
        nope = jnp.dot(latent, wk_ref[...], preferred_element_type=jnp.float32).astype(jnp.bfloat16)
        value = jnp.dot(latent, wv_ref[...], preferred_element_type=jnp.float32).astype(jnp.bfloat16)
        full = jnp.dot(
            query_ref[pl.ds(at, rows), :], wq_ref[...], preferred_element_type=jnp.float32
        )
        for part in range(rows // block):
            lo, hi = part * block, (part + 1) * block
            to = pl.multiple_of(order[step * (rows // block) + part] * block, block)
            there = pl.ds(to, block)
            cosine, sine = turn_ref[there, :ROPE], turn_ref[there, ROPE:]
            raw = rope_ref[pl.ds(pl.multiple_of(at + lo, block), block), :].astype(jnp.float32)
            key_rope = turned(raw, cosine, sine).astype(jnp.bfloat16)
            v_s[there, :] = value[lo:hi, :]
            for head in range(own):
                base = head * width
                k_s[head, there, :NOPE] = nope[lo:hi, head * NOPE : (head + 1) * NOPE]
                k_s[head, there, NOPE:] = key_rope
                q_s[head, there, :NOPE] = full[lo:hi, base : base + NOPE].astype(jnp.bfloat16)
                q_s[head, there, NOPE:] = turned(
                    full[lo:hi, base + NOPE : base + width], cosine, sine
                ).astype(jnp.bfloat16)
        return unused

    lax.fori_loop(0, count // rows, project, 0)

    def per_tile(number, best):
        opening = labels[number * tile]
        first = sum(
            (labels[(chunk + 1) * tile - 1] < opening).astype(jnp.int32)
            for chunk in range(count // tile)
        )
        own_labels = jnp.transpose(jnp.broadcast_to(row_ref[number], (tile, tile)))
        here = pl.ds(pl.multiple_of(number * tile, tile), tile)
        for head in range(own):
            m_s[head] = jnp.full((tile, 128), masked_value, jnp.float32)

        def score(chunk, unused):
            there = pl.ds(pl.multiple_of(chunk * tile, tile), tile)
            gap = (chunk - number) * tile
            later = lax.broadcasted_iota(jnp.int32, (tile, tile), 1) + gap
            now = lax.broadcasted_iota(jnp.int32, (tile, tile), 0)
            allowed = (later <= now) & (own_labels == row_ref[chunk])
            for head in range(own):
                raw = lax.dot_general(
                    q_s[head, here, :], k_s[head, there, :], (((1,), (1,)), ((), ())),
                    preferred_element_type=jnp.float32,
                )
                raw = jnp.where(allowed, raw, masked_value)
                s_s[chunk - first, head] = raw
                best_here = m_s[head]
                for lane in range(tile // 128):
                    best_here = jnp.maximum(best_here, raw[:, lane * 128 : (lane + 1) * 128])
                m_s[head] = best_here
            return unused

        lax.fori_loop(first, number + 1, score, 0)
        tops = []
        for head in range(own):
            top = jnp.max(m_s[head], axis=1, keepdims=True)
            m_s[head] = jnp.broadcast_to(top, (tile, 128))
            tops.append(jnp.broadcast_to(jnp.max(top, axis=0, keepdims=True), (1, 128)))

        factor = scale * math.log2(math.e)

        def mix(chunk, state):
            there = pl.ds(pl.multiple_of(chunk * tile, tile), tile)
            out = []
            for head in range(own):
                total, mixed = state[head]
                top = m_s[head]
                raw = s_s[chunk - first, head]
                pieces = [
                    jnp.exp2((raw[:, lane * 128 : (lane + 1) * 128] - top) * factor)
                    for lane in range(tile // 128)
                ]
                for piece in pieces:
                    total = total + piece
                weights = jnp.concatenate([piece.astype(jnp.bfloat16) for piece in pieces], axis=1)
                mixed = mixed + jnp.dot(
                    weights, v_s[there, head * VD : (head + 1) * VD],
                    preferred_element_type=jnp.float32,
                )
                out.append((total, mixed))
            return tuple(out)

        zero = tuple(
            (jnp.zeros((tile, 128), jnp.float32), jnp.zeros((tile, VD), jnp.float32))
            for head in range(own)
        )
        state = lax.fori_loop(first, number + 1, mix, zero)
        for head in range(own):
            total, mixed = state[head]
            done = (mixed / jnp.sum(total, axis=1, keepdims=True)).astype(jnp.bfloat16)
            for part in range(tile // block):
                to = pl.multiple_of(stored_at[number * (tile // block) + part] * block, block)
                context_ref[pl.ds(to, block), head * VD : (head + 1) * VD] = done[
                    part * block : (part + 1) * block, :
                ]
        return jnp.maximum(best, jnp.concatenate(tops, axis=0))

    best = lax.fori_loop(
        0, count // tile, per_tile, jnp.full((own, 128), masked_value, jnp.float32)
    )
    peak_ref[...] = best * scale


MESH = pl.DeviceIdType.MESH


def window(start, size):
    return pl.ds(pl.multiple_of(start * size, size), size)


def greet(wheres):
    barrier = pltpu.get_barrier_semaphore()
    for where in wheres:
        pl.semaphore_signal(barrier, inc=1, device_id=where, device_id_type=MESH)
    pl.semaphore_wait(barrier, len(wheres))


def spread(
    n, query_ref, key_ref, rope_ref, uq_ref, uk_ref, uv_ref,
    query_out, key_out, rope_out, wq_out, wk_out, wv_out,
    sends, got_query, got_key, got_rope, got_weight, local,
):
    s, t, d = lax.axis_index("seq"), lax.axis_index("tp"), lax.axis_index("dp")
    partner = s + 1 - 2 * lax.rem(s, 2)
    parity, level, levels = lax.rem(s, 2), s // 2, n // 2
    same = lambda z: 2 * z + parity
    cross = lambda z: 2 * z + 1 - parity
    turn = lambda k: lax.rem(level + k, levels)
    within = lambda z: (z >= 0) & (z < levels)
    beside, across, mate = {"tp": 1 - t}, {"dp": 1 - d}, {"seq": partner}
    greet(
        [mate, beside, across]
        + [{"seq": same(turn(k))} for k in range(1, levels)]
        + [{"seq": cross(turn(k))} for k in range(1, levels)]
    )
    rows, wide = query_ref.shape
    thin = key_ref.shape[1]
    weights = ((uq_ref, wq_out), (uk_ref, wk_out), (uv_ref, wv_out))
    state = {"when": None}
    started = []

    def link(source, target, arrived, where, sender):
        return pltpu.make_async_remote_copy(
            src_ref=source, dst_ref=target, send_sem=sends.at[sender], recv_sem=arrived,
            device_id=where, device_id_type=MESH,
        )

    def send(source, target, arrived, where):
        link(source, target, arrived, where, len(started)).start()
        started.append((tuple(source.shape), state["when"]))

    def under(condition, action):
        state["when"] = condition
        pl.when(condition)(action)
        state["when"] = None

    def arrive(target, arrived):
        link(target, target, arrived, mate, 0).wait_recv()

    def spots(src, tp):
        return (
            (query_out.at[window(src, rows), window(tp, wide)], got_query.at[src, tp]),
            (key_out.at[window(src, rows), window(tp, thin)], got_key.at[src, tp]),
        )

    def rope_spot(src):
        return (rope_out.at[window(src, rows), :], got_rope.at[src])

    def own_latents(where, rope):
        for source, (target, arrived) in zip((query_ref, key_ref), spots(s, t)):
            send(source, target, arrived, where)
        if rope:
            send(rope_ref, *rope_spot(s), where)

    def await_latents(src, tp, rope):
        for target, arrived in spots(src, tp):
            arrive(target, arrived)
        if rope:
            arrive(*rope_spot(src))

    def pass_latents(src, tp, where, rope):
        for target, arrived in spots(src, tp):
            send(target, target, arrived, where)
        if rope:
            target, arrived = rope_spot(src)
            send(target, target, arrived, where)

    def weight_spot(index, src, half):
        out = weights[index][1]
        depth = weights[index][0].shape[0] // 2
        return (out.at[window(src * 2 + half, depth), :], got_weight.at[index, src, half])

    def own_weights(to):
        for index, (ref, out) in enumerate(weights):
            piece = ref.at[window(d, ref.shape[0] // 2), window(to, out.shape[1])]
            send(piece, *weight_spot(index, s, d), {"seq": to})

    def pass_weights(src):
        for index in range(len(weights)):
            target, arrived = weight_spot(index, src, d)
            arrive(target, arrived)
            send(target, target, arrived, across)

    own_latents(beside, False)
    for sign in (1, -1):
        to = level + sign
        under(within(to), lambda: own_latents({"seq": same(to)}, True))
    own_latents(mate, True)
    own_weights(partner)
    kept = [
        pltpu.make_async_copy(source, target, local.at[place])
        for place, (source, target) in enumerate(
            [(query_ref, spots(s, t)[0][0]), (key_ref, spots(s, t)[1][0]), (rope_ref, rope_spot(s)[0])]
            + [
                (ref.at[:, window(s, out.shape[1])], out.at[window(s, ref.shape[0]), :])
                for ref, out in weights
            ]
        )
    ]
    for copy in kept:
        copy.start()

    def from_beside(k):
        for sign in (1, -1) if k else (1,):
            source = level - sign * k

            def hand():
                await_latents(same(source), 1 - t, False)
                pass_latents(same(source), 1 - t, mate, False)

            under(within(source), hand)

    for k in range(1, levels):
        for sign in (1, -1):
            to = level + sign * k

            def far():
                own_weights(same(to))
                own_weights(cross(to))

            under(within(to), far)
        for sign in (1, -1):
            source, onward = level - sign * k, level + sign

            def take():
                await_latents(same(source), t, True)
                pass_latents(same(source), t, beside, False)
                pass_latents(same(source), t, mate, True)

            under(within(source), take)
            under(
                within(source) & within(onward),
                lambda: pass_latents(same(source), t, {"seq": same(onward)}, True),
            )
        if k == 1:
            pass_weights(partner)
        for sign in (1, -1):
            source = level - sign * k

            def relay():
                pass_weights(same(source))
                pass_weights(cross(source))

            under(within(source), relay)
        from_beside(k - 1)
    from_beside(levels - 1)
    for k in range(levels):
        await_latents(cross(turn(k)), t, True)
        await_latents(cross(turn(k)), 1 - t, False)
    for k in range(levels):
        for src in [cross(turn(k))] + ([same(turn(k))] if k else []):
            for index in range(len(weights)):
                arrive(*weight_spot(index, src, 1 - d))
    alike = [target for target, _ in spots(s, t)] + [rope_spot(s)[0]]
    alike += [weight_spot(index, s, d)[0] for index in range(len(weights))]
    alike = {tuple(ref.shape): ref for ref in alike}
    for sender, (shape, condition) in enumerate(started):
        sent = link(alike[shape], alike[shape], got_rope.at[s], mate, sender)
        if condition is None:
            sent.wait_send()
        else:
            pl.when(condition)(sent.wait_send)
    for copy in kept:
        copy.wait()


def give_back(n, context_ref, peak_ref, out_ref, peaks_ref, sends, got_context, got_peak, local):
    s, d = lax.axis_index("seq"), lax.axis_index("dp")
    rows, wide = out_ref.shape[0], context_ref.shape[1]
    steps = [k for k in range(1, n)]
    peers = [lax.rem(s + k, n) for k in steps]
    wheres = [{"seq": to} for to in peers]
    others = [{"dp": 1 - d}] + [{"seq": to, "dp": 1 - d} for to in peers]
    greet(wheres + others)
    started = []

    def link(source, target, arrived, where, sender):
        return pltpu.make_async_remote_copy(
            src_ref=source, dst_ref=target, send_sem=sends.at[sender], recv_sem=arrived,
            device_id=where, device_id_type=MESH,
        )

    def send(source, target, arrived, where):
        copy = link(source, target, arrived, where, len(started))
        copy.start()
        started.append(copy)

    me = d * n + s
    for where in wheres + others:
        send(peak_ref, peaks_ref.at[me], got_peak.at[me], where)
    for to, where in zip(peers, wheres):
        send(context_ref.at[window(to, rows), :], out_ref.at[:, window(s, wide)], got_context.at[s], where)
    kept = [
        pltpu.make_async_copy(peak_ref, peaks_ref.at[me], local.at[0]),
        pltpu.make_async_copy(context_ref.at[window(s, rows), :], out_ref.at[:, window(s, wide)], local.at[1]),
    ]
    for copy in kept:
        copy.start()
    for src in peers:
        target = out_ref.at[:, window(src, wide)]
        link(target, target, got_context.at[src], wheres[0], 0).wait_recv()
    for src in [d * n + p for p in peers] + [(1 - d) * n + p for p in peers] + [(1 - d) * n + s]:
        link(peaks_ref.at[src], peaks_ref.at[src], got_peak.at[src], wheres[0], 0).wait_recv()
    for copy in started:
        copy.wait_send()
    for copy in kept:
        copy.wait()


def by_heads(query_latent, key_latent, rope_key, w_uq, w_uk, w_uv, block_order, segment_ids):
    devices = lax.axis_size("seq")
    heads = w_uq.shape[1] // (NOPE + ROPE)
    own = heads // devices
    anyplace = pl.BlockSpec(memory_space=pl.ANY)
    vmem = pl.BlockSpec(memory_space=pltpu.VMEM)
    smem = pl.BlockSpec(memory_space=pltpu.SMEM)
    sides = lax.axis_size("tp")
    rows = query_latent.shape[1]
    shapes = (
        (devices * rows, sides * query_latent.shape[2]),
        (devices * rows, sides * key_latent.shape[2]),
        (devices * rows, ROPE),
        (devices * w_uq.shape[0], w_uq.shape[1] // devices),
        (devices * w_uk.shape[0], w_uk.shape[1] // devices),
        (devices * w_uv.shape[0], w_uv.shape[1] // devices),
    )
    half = devices // 2
    copies = 44 * half
    query, key, rope, wq, wk, wv = pl.pallas_call(
        functools.partial(spread, devices),
        out_shape=[jax.ShapeDtypeStruct(shape, jnp.bfloat16) for shape in shapes],
        in_specs=[anyplace] * 6,
        out_specs=[anyplace] * 6,
        scratch_shapes=[
            pltpu.SemaphoreType.DMA((copies,)),
            pltpu.SemaphoreType.DMA((devices, sides)),
            pltpu.SemaphoreType.DMA((devices, sides)),
            pltpu.SemaphoreType.DMA((devices,)),
            pltpu.SemaphoreType.DMA((3, devices, 2)),
            pltpu.SemaphoreType.DMA((6,)),
        ],
        compiler_params=pltpu.CompilerParams(collective_id=0, has_side_effects=True),
        cost_estimate=pl.CostEstimate(
            flops=30_000_000_000, bytes_accessed=16_000_000, transcendentals=0
        ),
        name="spread",
    )(query_latent[0], key_latent[0], rope_key[0], w_uq, w_uk, w_uv)
    order, labels = block_order[0], segment_ids[0]
    count, blocks = labels.shape[0], order.shape[0]
    block = count // blocks
    tile = 2 * block
    chunks = count // tile
    steps = np.arange(ROPE // 2, dtype=np.float32) * np.float32(2.0 / ROPE)
    freqs = np.exp(np.float32(-math.log(rope_base)) * steps).astype(np.float32)
    angle = np.arange(count, dtype=np.float32)[:, None] * freqs[None, :]
    cosine, sine = np.cos(angle), np.sin(angle)
    turns = jnp.asarray(np.concatenate([cosine, cosine, -sine, sine], axis=1), jnp.float32)
    context, peak = pl.pallas_call(
        functools.partial(attend, block, tile, own),
        out_shape=(
            jax.ShapeDtypeStruct((count, own * VD), jnp.bfloat16),
            jax.ShapeDtypeStruct((own, 128), jnp.float32),
        ),
        in_specs=[smem] * 2 + [vmem] * 8,
        out_specs=(vmem, vmem),
        scratch_shapes=[
            pltpu.VMEM((own, count, NOPE + ROPE), jnp.bfloat16),
            pltpu.VMEM((own, count, NOPE + ROPE), jnp.bfloat16),
            pltpu.VMEM((count, own * VD), jnp.bfloat16),
            pltpu.VMEM((chunks, own, tile, tile), jnp.float32),
            pltpu.VMEM((own, tile, 128), jnp.float32),
            pltpu.SMEM((blocks,), jnp.int32),
        ],
        compiler_params=pltpu.CompilerParams(vmem_limit_bytes=60 * 1024 * 1024),
        cost_estimate=pl.CostEstimate(
            flops=12_000_000_000, bytes_accessed=16_000_000, transcendentals=4_000_000
        ),
        name="attend",
    )(
        order, labels, query, key, rope, wq, wk, wv, turns, labels.reshape(chunks, 1, tile),
    )
    context, peaks = pl.pallas_call(
        functools.partial(give_back, devices),
        out_shape=[
            jax.ShapeDtypeStruct((rows, heads * VD), jnp.bfloat16),
            jax.ShapeDtypeStruct((2 * devices, own, 128), jnp.float32),
        ],
        in_specs=[anyplace, vmem],
        out_specs=[anyplace, vmem],
        scratch_shapes=[
            pltpu.SemaphoreType.DMA((3 * devices,)),
            pltpu.SemaphoreType.DMA((devices,)),
            pltpu.SemaphoreType.DMA((2 * devices,)),
            pltpu.SemaphoreType.DMA((2,)),
        ],
        compiler_params=pltpu.CompilerParams(collective_id=1, has_side_effects=True),
        name="give_back",
    )(context, peak)
    head_max = jnp.max(peaks[:, :, 0].reshape(2, heads), axis=0)
    return (context[None],) + clipped(w_uq, w_uk, head_max, heads)


def clipped(w_uq, w_uk, head_max, heads):
    ratio = CLIP / jnp.maximum(head_max, CLIP)
    root = jnp.sqrt(ratio)
    factors = jnp.concatenate(
        [
            jnp.broadcast_to(root[:, None], (heads, NOPE)),
            jnp.broadcast_to(ratio[:, None], (heads, ROPE)),
        ],
        axis=1,
    ).reshape(heads * (NOPE + ROPE))
    clipped_uq = (w_uq.astype(jnp.float32) * factors[None, :]).astype(jnp.bfloat16)
    clipped_uk = (w_uk.astype(jnp.float32) * jnp.repeat(root, NOPE)[None, :]).astype(jnp.bfloat16)
    return (clipped_uq, clipped_uk)


def on_device(*arrays):
    heads = arrays[3].shape[1] // (NOPE + ROPE)
    pairs = lax.axis_size("tp") == 2 and lax.axis_size("dp") == 2
    if pairs and heads % (2 * lax.axis_size("seq")) == 0:
        return by_heads(*arrays)
    return by_tokens(*arrays)


def solution(mesh):
    placed = (
        P("dp", "seq", "tp"),
        P("dp", "seq", "tp"),
        P("dp", "seq", None),
        P("seq", "tp"),
        P("seq", "tp"),
        P("seq", "tp"),
        P("dp", None),
        P("dp", None),
    )
    return jax.shard_map(
        on_device,
        mesh=mesh,
        in_specs=placed,
        out_specs=(P("dp", "seq", "tp"), P("seq", "tp"), P("seq", "tp")),
        check_vma=False,
    )
```
